128 devices in a mesh: group: 4 (over x_lo, core), blk: 32 (over y, z, x_hi).
Axes of the slice: x: 4 (x_hi: 2, x_lo: 2; x = x_hi * 2 + x_lo), y: 4, z: 4, core: 2. Of those that a mesh axis runs over, the one named last changes fastest.
Arguments:
- orbitals: float32 [128, 64, 4096], P(('group', 'blk')), may hold values from -6 to 6
- occupation: float32 [128], P(('group', 'blk')), may hold values from 0.3 to 1
Outputs:
- exchange: float32 [128, 64, 4096], P(('group', 'blk'))
The draws below stay inside these ranges and needn't reach their ends.
All inputs are finite; a program needn't handle non-finite values.
Results may differ from the reference program's by a relative error of at most 0.0003.
Values sent between devices are 32-bit elements; how exact they have to be, the bound alone decides.
No kernel may reach another device: no remote copies, remote signals or barrier semaphores. Data moves between devices by JAX's collectives and lax.ppermute only.
A program may use at most 128 MiB of HBM per device.

```python
import jax
import jax.numpy as jnp
from jax import lax

GRID = 64
ORB_DEV = 1
STEPS = 3
ORBITALS = 128
N_GROUP = 4
N_BLK = 32


def block_scale(key, dims, shards, smallest, largest):
    def one(dim, parts):
        draws = jax.random.uniform(jax.random.fold_in(jax.random.fold_in(key, 6), dim), (parts,), jnp.float32, smallest / len(shards), largest / len(shards))
        return jnp.repeat(jnp.exp(draws), dims[dim] // parts).reshape((-1,) + (1,) * (len(dims) - dim - 1))

    gain = one(*shards[0])
    for cut in shards[1:]:
        gain = gain * one(*cut)
    return gain


def normal_values(stream_key, extent, width, reach, shards=(), kind=jnp.bfloat16):
    factor_of = block_scale(stream_key, extent, shards, -0.22, 0.18) if shards else 1.0
    values = jax.random.normal(stream_key, extent, jnp.float32) * width * factor_of
    return jnp.minimum(jnp.maximum(values, -reach), reach).astype(kind)


def setup_inputs(seed: int = 0) -> dict:
    keys = jax.random.split(jax.random.key(seed), 3)
    return {
        "orbitals": normal_values(keys[0], (ORBITALS, GRID, GRID * GRID), 1.0, 6.0, ((0, 128),), jnp.float32),
        "occupation": jnp.clip(0.3 + 0.7 * jax.random.uniform(keys[1], (ORBITALS,), jnp.float32) ** block_scale(keys[1], (ORBITALS,), ((0, 128),), -0.2, 0.2), 0.3, 1.0),
    }


def make_kernel(size):
    index = jnp.arange(size)
    signed = jnp.where(index < size // 2, index, index - size).astype(jnp.float32)
    square = signed * signed
    total = square[:, None, None] + square[None, :, None] + square[None, None, :]
    step = 2.0 * jnp.pi / size
    return jnp.pi / (step * step * total + 0.25)


def pair_terms(home, home_occ, visit, visit_occ, kernel):
    size = home.shape[1]
    count = home.shape[0]
    density = home[:, None] * visit[None, :]
    cube = density.reshape(count, count, size, size, size)
    freq = jnp.fft.fftn(cube, axes=(2, 3, 4))
    potential = jnp.real(jnp.fft.ifftn(freq * kernel, axes=(2, 3, 4)))
    potential = potential.reshape(count, count, size, size * size).astype(jnp.float32)
    home_term = -jnp.sum(visit_occ[None, :, None, None] * visit[None, :] * potential, axis=1)
    visit_term = -jnp.sum(home_occ[:, None, None, None] * home[:, None] * potential, axis=0)
    return home_term, visit_term


def reference(orbitals, occupation):
    size = orbitals.shape[1]
    count = ORB_DEV
    blocks = orbitals.reshape(N_GROUP * N_BLK, count, size, size * size)
    occ_blocks = occupation.reshape(N_GROUP * N_BLK, count)
    kernel = make_kernel(size)

    def one_block(acc, home_index):
        group_index = home_index // N_BLK
        place = home_index % N_BLK
        home = blocks[home_index]
        home_occ = occ_blocks[home_index]
        partners = []
        for shift in range(1, STEPS + 1):
            partners.append(group_index * N_BLK + (place - shift) % N_BLK)
        partners.append(((group_index - 1) % N_GROUP) * N_BLK + (place - STEPS) % N_BLK)
        for partner in partners:
            partner = partner.astype(jnp.int32)
            visit = blocks[partner]
            visit_occ = occ_blocks[partner]
            home_term, visit_term = pair_terms(home, home_occ, visit, visit_occ, kernel)
            acc = acc.at[home_index].add(home_term)
            acc = acc.at[partner].add(visit_term)
        return acc, None

    start = jnp.zeros(blocks.shape, jnp.float32)
    result, _ = lax.scan(one_block, start, jnp.arange(N_GROUP * N_BLK, dtype=jnp.int32))
    return result.reshape(orbitals.shape)
```

```python
import jax
import jax.numpy as jnp
import numpy as np
from jax import lax
from jax.experimental import pallas as pl
from jax.experimental.pallas import tpu as pltpu
from jax.sharding import PartitionSpec as P

SIZE = 64
HALF = 32
ROWS = 36
BF = jnp.bfloat16
F32 = jnp.float32


def two_parts(matrix):
    high = np.asarray(matrix, np.float64).astype(BF)
    low = (np.asarray(matrix, np.float64) - high.astype(np.float64)).astype(BF)
    return high, low


def real_basis(points, freqs, period):
    place = np.arange(points)
    rows, marks = [], []
    for freq in freqs:
        waves = [np.cos(2 * np.pi * freq * place / period)]
        waves.append(np.sin(2 * np.pi * freq * place / period))
        for wave in waves:
            norm = np.sqrt(np.sum(wave * wave))
            if norm > 1e-6:
                rows.append(wave / norm)
                marks.append(freq)
    return np.stack(rows), np.asarray(marks, np.float64)


def left_form(matrix):
    high, low = two_parts(matrix)
    return np.concatenate([high, high, low], axis=1)


def right_form(matrix):
    high, low = two_parts(matrix)
    row = np.concatenate([high, low], axis=1)
    return np.concatenate([row, row], axis=0)


def constants():
    full, marks = real_basis(SIZE, range(HALF + 1), SIZE)
    even, even_marks = real_basis(HALF, range(0, HALF + 1, 2), SIZE)
    odd, odd_marks = real_basis(HALF, range(1, HALF, 2), SIZE)
    mix = np.array([[1.0, 1.0], [1.0, -1.0]]) / np.sqrt(2.0)
    lane = np.kron(mix, full)
    mid_marks = np.stack([even_marks, odd_marks], axis=1)
    total = (
        marks[:, None, None, None] ** 2
        + mid_marks[None, :, :, None] ** 2
        + marks[None, None, None, :] ** 2
    )
    step = 2.0 * np.pi / SIZE
    kernel = (np.pi / (step * step * total + 0.25)).astype(np.float32)
    kernel = kernel.reshape(SIZE * HALF, 2 * SIZE)
    return (
        left_form(full),
        left_form(full.T),
        right_form(lane.T),
        right_form(lane),
        left_form(np.concatenate([even, odd], axis=0)),
        left_form(np.concatenate([even.T, odd.T], axis=0)),
        kernel,
    )


def split(value):
    high = value.astype(BF)
    low = (value - high.astype(F32)).astype(BF)
    return high, low


def along_rows(matrix, value):
    high, low = split(value)
    stack = jnp.concatenate([high, low, high], axis=0)
    return jnp.dot(matrix, stack, preferred_element_type=F32)


def along_lanes(value, matrix):
    high, low = split(value)
    both = jnp.dot(
        jnp.concatenate([high, low], axis=1), matrix, preferred_element_type=F32
    )
    return both[:, :128] + both[:, 128:]


def to_rows(value):
    count = value.shape[1] // 128
    return jnp.concatenate(
        [value[:, n * 128 : (n + 1) * 128] for n in range(count)], axis=0
    )


def to_lanes(value, rows):
    count = value.shape[0] // rows
    return jnp.concatenate(
        [value[n * rows : (n + 1) * rows] for n in range(count)], axis=1
    )


def pick(value):
    lane = lax.broadcasted_iota(jnp.int32, (HALF, value.shape[1]), 1)
    return jnp.where((lane & 127) < SIZE, value[:HALF], value[HALF:])


def forward(left, right, mats, area, tiles=8):
    fa, _, fl, _, _, _, _ = mats
    for base in range(0, HALF, tiles):
        lanes = pl.ds(base * 128, tiles * 128)
        value = along_rows(fa[...], left[:, lanes] * right[:, lanes])
        value = along_lanes(to_rows(value), fl[...])
        for n in range(tiles):
            area[pl.ds(base + n, SIZE, stride=ROWS), :] = value[n * SIZE : (n + 1) * SIZE]


def middle(mats, area, count=8):
    _, _, _, _, fm, bm, kernel = mats
    for base in range(0, SIZE, count):
        value = jnp.concatenate(
            [area[pl.ds((base + n) * ROWS, HALF), :] for n in range(count)], axis=1
        )
        value = pick(along_rows(fm[...], value))
        value = value * to_lanes(kernel[pl.ds(base * HALF, count * HALF), :], HALF)
        value = pick(along_rows(bm[...], value))
        for n in range(count):
            area[pl.ds((base + n) * ROWS, HALF), :] = value[:, n * 128 : (n + 1) * 128]


def backward(mats, area, base, tiles=8):
    _, ba, _, bl, _, _, _ = mats
    value = jnp.concatenate(
        [area[pl.ds(base + n, SIZE, stride=ROWS), :] for n in range(tiles)], axis=0
    )
    value = along_lanes(value, bl[...])
    return along_rows(ba[...], to_lanes(value, SIZE))


def pack_body(occ, orb, out):
    scale = jnp.sqrt(jnp.full((1, 128), occ[0], F32))
    low = lax.broadcasted_iota(jnp.int32, (SIZE, 128), 1) < SIZE
    for n in range(HALF // 2):
        first = orb[:, n * 128 : (n + 1) * 128] * scale
        second = orb[:, (n + 16) * 128 : (n + 17) * 128] * scale
        even = jnp.where(low, first, pltpu.roll(second, SIZE, 1))
        odd = jnp.where(low, pltpu.roll(first, SIZE, 1), second)
        out[:, 2 * n * 128 : (2 * n + 1) * 128] = even
        out[:, (2 * n + 1) * 128 : (2 * n + 2) * 128] = odd


def unpack_body(occ, one, two, three, out):
    scale = -lax.rsqrt(jnp.full((1, 128), occ[0], F32))
    low = lax.broadcasted_iota(jnp.int32, (SIZE, 128), 1) < SIZE
    for n in range(HALF // 2):
        parts = []
        for m in (2 * n, 2 * n + 1):
            lanes = slice(m * 128, (m + 1) * 128)
            parts.append((one[:, lanes] + two[:, lanes] + three[:, lanes]) * scale)
        even, odd = parts
        out[:, n * 128 : (n + 1) * 128] = jnp.where(low, even, pltpu.roll(odd, SIZE, 1))
        out[:, (n + 16) * 128 : (n + 17) * 128] = jnp.where(
            low, pltpu.roll(even, SIZE, 1), odd
        )


SHAPE = jax.ShapeDtypeStruct((SIZE, SIZE * SIZE), F32)
SMEM = pl.BlockSpec(memory_space=pltpu.SMEM)
VMEM = pl.BlockSpec(memory_space=pltpu.VMEM)
COST = 2 * 6 * SIZE**4 * 200


def call(body, name, outs, scratch=(), work=1, first=VMEM, count=1, limit=20):
    return pl.pallas_call(
        body,
        out_shape=[SHAPE] * outs,
        in_specs=[first] + [VMEM] * (count - 1),
        out_specs=[VMEM] * outs,
        scratch_shapes=list(scratch),
        cost_estimate=pl.CostEstimate(
            flops=work * COST, bytes_accessed=1 << 20, transcendentals=0
        ),
        compiler_params=pltpu.CompilerParams(vmem_limit_bytes=limit << 20),
        name=name,
    )


def three_body(left, home, right, *rest):
    mats, outs, area = rest[:7], rest[7:10], rest[10]
    refs = (left, home, right)
    fresh = [True] * 3
    for one, two in ((1, 2), (0, 1), (0, 2)):
        forward(refs[one], refs[two], mats, area)
        middle(mats, area)
        for base in range(0, HALF, 8):
            value = backward(mats, area, base)
            lanes = pl.ds(base * 128, 1024)
            for own, other in ((one, two), (two, one)):
                term = value * refs[other][:, lanes]
                if fresh[own]:
                    outs[own][:, lanes] = term
                else:
                    outs[own][:, lanes] += term
        fresh[one] = fresh[two] = False


def last_body(left, far, acc, *rest):
    mats, outs, area = rest[:7], rest[7:9], rest[9]
    forward(left, far, mats, area)
    middle(mats, area)
    for base in range(0, HALF, 8):
        value = backward(mats, area, base)
        lanes = pl.ds(base * 128, 1024)
        outs[0][:, lanes] = acc[:, lanes] + value * far[:, lanes]
        outs[1][:, lanes] = value * left[:, lanes]


def shift(value, axis, steps):
    count = lax.axis_size(axis)
    pairs = [(source, (source + steps) % count) for source in range(count)]
    return lax.ppermute(value, axis, pairs)


def local(orbitals, occupation):
    mats = [jnp.asarray(item) for item in constants()]
    area = [pltpu.VMEM((SIZE * ROWS, 128), F32)]
    home = call(pack_body, "pack", 1, first=SMEM, count=2, work=0)(
        occupation, orbitals[0]
    )[0]
    left = shift(home, "blk", -1)
    right = shift(home, "blk", 2)
    far = shift(right, "group", 1)
    acc_left, acc_home, acc_right = call(three_body, "three", 3, area, 3, count=10)(
        left, home, right, *mats
    )
    acc_left, acc_far = call(last_body, "last", 2, area, 1, count=10)(
        left, far, acc_left, *mats
    )
    from_far = shift(acc_far, "group", -1)
    from_left = shift(acc_left, "blk", 1)
    from_right = shift(acc_right + from_far, "blk", -2)
    out = call(unpack_body, "unpack", 1, first=SMEM, count=4, work=0)(
        occupation, acc_home, from_left, from_right
    )[0]
    return out[None]


def solution(mesh):
    spec = P(("group", "blk"))
    return jax.shard_map(
        local,
        mesh=mesh,
        in_specs=(P(("group", "blk"), None, None), spec),
        out_specs=P(("group", "blk"), None, None),
        check_vma=False,
    )
```

```python
import jax
import jax.numpy as jnp
import numpy as np
from jax import lax
from jax.experimental import pallas as pl
from jax.experimental.pallas import tpu as pltpu
from jax.sharding import PartitionSpec as P

SIZE = 64
HALF = 32
ROWS = 36
BF = jnp.bfloat16
F32 = jnp.float32


def two_parts(matrix):
    high = np.asarray(matrix, np.float64).astype(BF)
    low = (np.asarray(matrix, np.float64) - high.astype(np.float64)).astype(BF)
    return high, low


def real_basis(points, freqs, period):
    place = np.arange(points)
    rows, marks = [], []
    for freq in freqs:
        waves = [np.cos(2 * np.pi * freq * place / period)]
        waves.append(np.sin(2 * np.pi * freq * place / period))
        for wave in waves:
            norm = np.sqrt(np.sum(wave * wave))
            if norm > 1e-6:
                rows.append(wave / norm)
                marks.append(freq)
    return np.stack(rows), np.asarray(marks, np.float64)


def left_form(matrix):
    high, low = two_parts(matrix)
    return np.concatenate([high, high, low], axis=1)


def right_form(matrix):
    high, low = two_parts(matrix)
    row = np.concatenate([high, low], axis=1)
    return np.concatenate([row, row], axis=0)


def constants():
    full, marks = real_basis(SIZE, range(HALF + 1), SIZE)
    even, even_marks = real_basis(HALF, range(0, HALF + 1, 2), SIZE)
    odd, odd_marks = real_basis(HALF, range(1, HALF, 2), SIZE)
    mix = np.array([[1.0, 1.0], [1.0, -1.0]]) / np.sqrt(2.0)
    lane = np.kron(mix, full)
    mid_marks = np.stack([even_marks, odd_marks], axis=1)
    total = (
        marks[:, None, None, None] ** 2
        + mid_marks[None, :, :, None] ** 2
        + marks[None, None, None, :] ** 2
    )
    step = 2.0 * np.pi / SIZE
    kernel = (np.pi / (step * step * total + 0.25)).astype(np.float32)
    kernel = kernel.reshape(SIZE * HALF, 2 * SIZE)
    return (
        left_form(full),
        left_form(full.T),
        right_form(lane.T),
        right_form(lane),
        left_form(np.concatenate([even, odd], axis=0)),
        left_form(np.concatenate([even.T, odd.T], axis=0)),
        kernel,
    )


def split(value):
    high = value.astype(BF)
    low = (value - high.astype(F32)).astype(BF)
    return high, low


def along_rows(matrix, value):
    high, low = split(value)
    stack = jnp.concatenate([high, low, high], axis=0)
    return jnp.dot(matrix, stack, preferred_element_type=F32)


def along_lanes(value, matrix):
    high, low = split(value)
    both = jnp.dot(
        jnp.concatenate([high, low], axis=1), matrix, preferred_element_type=F32
    )
    return both[:, :128] + both[:, 128:]


def to_rows(value):
    count = value.shape[1] // 128
    return jnp.concatenate(
        [value[:, n * 128 : (n + 1) * 128] for n in range(count)], axis=0
    )


def to_lanes(value, rows):
    count = value.shape[0] // rows
    return jnp.concatenate(
        [value[n * rows : (n + 1) * rows] for n in range(count)], axis=1
    )


def pick(value):
    lane = lax.broadcasted_iota(jnp.int32, (HALF, value.shape[1]), 1)
    return jnp.where((lane & 127) < SIZE, value[:HALF], value[HALF:])


def take(refs, lanes):
    parts = [ref[:, lanes] for ref in refs]
    return parts[0] if len(parts) == 1 else jnp.concatenate(parts, axis=0)


def put(refs, lanes, value):
    refs[0][:, lanes] = value[:HALF]
    refs[1][:, lanes] = value[HALF:]


def forward(left, right, mats, area, tiles=8):
    fa, _, fl, _, _, _, _ = mats
    for base in range(0, HALF, tiles):
        lanes = pl.ds(base * 128, tiles * 128)
        value = along_rows(fa[...], take(left, lanes) * take(right, lanes))
        value = along_lanes(to_rows(value), fl[...])
        for n in range(tiles):
            area[pl.ds(base + n, SIZE, stride=ROWS), :] = value[n * SIZE : (n + 1) * SIZE]


def middle(mats, area, count=8):
    _, _, _, _, fm, bm, kernel = mats
    for base in range(0, SIZE, count):
        value = jnp.concatenate(
            [area[pl.ds((base + n) * ROWS, HALF), :] for n in range(count)], axis=1
        )
        value = pick(along_rows(fm[...], value))
        value = value * to_lanes(kernel[pl.ds(base * HALF, count * HALF), :], HALF)
        value = pick(along_rows(bm[...], value))
        for n in range(count):
            area[pl.ds((base + n) * ROWS, HALF), :] = value[:, n * 128 : (n + 1) * 128]


def backward(mats, area, base, tiles=8):
    _, ba, _, bl, _, _, _ = mats
    value = jnp.concatenate(
        [area[pl.ds(base + n, SIZE, stride=ROWS), :] for n in range(tiles)], axis=0
    )
    value = along_lanes(value, bl[...])
    return along_rows(ba[...], to_lanes(value, SIZE))

def pack_body(occ, orb, out, top, bottom):
    scale = jnp.sqrt(jnp.full((1, 128), occ[0], F32))
    low = lax.broadcasted_iota(jnp.int32, (SIZE, 128), 1) < SIZE
    for n in range(HALF // 2):
        first = orb[:, n * 128 : (n + 1) * 128] * scale
        second = orb[:, (n + 16) * 128 : (n + 17) * 128] * scale
        even = jnp.where(low, first, pltpu.roll(second, SIZE, 1))
        odd = jnp.where(low, pltpu.roll(first, SIZE, 1), second)
        for m, value in ((2 * n, even), (2 * n + 1, odd)):
            lanes = slice(m * 128, (m + 1) * 128)
            out[:, lanes] = value
            top[:, lanes] = value[:HALF]
            bottom[:, lanes] = value[HALF:]


def unpack_body(occ, one, two, top, bottom, out):
    scale = -lax.rsqrt(jnp.full((1, 128), occ[0], F32))
    low = lax.broadcasted_iota(jnp.int32, (SIZE, 128), 1) < SIZE
    for n in range(HALF // 2):
        parts = []
        for m in (2 * n, 2 * n + 1):
            lanes = slice(m * 128, (m + 1) * 128)
            three = take((top, bottom), lanes)
            parts.append((one[:, lanes] + two[:, lanes] + three) * scale)
        even, odd = parts
        out[:, n * 128 : (n + 1) * 128] = jnp.where(low, even, pltpu.roll(odd, SIZE, 1))
        out[:, (n + 16) * 128 : (n + 17) * 128] = jnp.where(
            low, pltpu.roll(even, SIZE, 1), odd
        )


WHOLE = jax.ShapeDtypeStruct((SIZE, SIZE * SIZE), F32)
PART = jax.ShapeDtypeStruct((HALF, SIZE * SIZE), F32)
SMEM = pl.BlockSpec(memory_space=pltpu.SMEM)
VMEM = pl.BlockSpec(memory_space=pltpu.VMEM)
COST = 2 * 6 * SIZE**4 * 200
AREA = pltpu.VMEM((SIZE * ROWS, 128), F32)


def call(body, name, count, outs, scratch=(), work=0, first=VMEM):
    return pl.pallas_call(
        body,
        out_shape=list(outs),
        in_specs=[first] + [VMEM] * (count - 1),
        out_specs=[VMEM] * len(outs),
        scratch_shapes=list(scratch),
        cost_estimate=pl.CostEstimate(
            flops=work * COST, bytes_accessed=1 << 20, transcendentals=0
        ),
        compiler_params=pltpu.CompilerParams(vmem_limit_bytes=20 << 20),
        name=name,
    )


def edge(one, two, mats, area, finish):
    forward(one, two, mats, area)
    middle(mats, area)
    for base in range(0, HALF, 8):
        value = backward(mats, area, base)
        lanes = pl.ds(base * 128, 1024)
        finish(lanes, value * take(two, lanes), value * take(one, lanes))


def right_body(home, top, bottom, *rest):
    mats, (home_out, top_out, bottom_out, area) = rest[:7], rest[7:]

    def finish(lanes, first, second):
        home_out[:, lanes] = first
        put((top_out, bottom_out), lanes, second)

    edge((home,), (top, bottom), mats, area, finish)


def far_body(left, top, bottom, *rest):
    mats, (left_out, top_out, bottom_out, area) = rest[:7], rest[7:]

    def finish(lanes, first, second):
        left_out[:, lanes] = first
        put((top_out, bottom_out), lanes, second)

    edge((left,), (top, bottom), mats, area, finish)


def left_body(left, home, top, bottom, left_in, home_in, top_in, bottom_in, *rest):
    mats, outs = rest[:7], rest[7:]
    left_out, home_out, top_out, bottom_out, area = outs

    def finish_home(lanes, first, second):
        left_out[:, lanes] = left_in[:, lanes] + first
        home_out[:, lanes] = home_in[:, lanes] + second

    def finish_right(lanes, first, second):
        left_out[:, lanes] += first
        put((top_out, bottom_out), lanes, take((top_in, bottom_in), lanes) + second)

    edge((left,), (home,), mats, area, finish_home)
    edge((left,), (top, bottom), mats, area, finish_right)


def shift(value, axis, steps):
    count = lax.axis_size(axis)
    pairs = [(source, (source + steps) % count) for source in range(count)]
    return lax.ppermute(value, axis, pairs)


def local(orbitals, occupation):
    mats = [jnp.asarray(item) for item in constants()]
    pair = [WHOLE, PART, PART]
    home, top, bottom = call(pack_body, "pack", 2, pair, first=SMEM)(
        occupation, orbitals[0]
    )
    right = [shift(part, "blk", 2) for part in (top, bottom)]
    left = shift(home, "blk", -1)
    far = [shift(part, "group", 1) for part in right]
    acc_home, *acc_right = call(right_body, "right", 10, pair, [AREA], 1)(
        home, *right, *mats
    )
    acc_left, *acc_far = call(far_body, "far", 10, pair, [AREA], 1)(
        left, *far, *mats
    )
    from_far = [shift(part, "group", -1) for part in acc_far]
    acc_left, acc_home, *acc_right = call(
        left_body, "left", 15, [WHOLE, WHOLE, PART, PART], [AREA], 2
    )(left, home, *right, acc_left, acc_home, *acc_right, *mats)
    from_left = shift(acc_left, "blk", 1)
    from_right = [
        shift(one + two, "blk", -2) for one, two in zip(acc_right, from_far)
    ]
    out = call(unpack_body, "unpack", 5, [WHOLE], first=SMEM)(
        occupation, acc_home, from_left, *from_right
    )[0]
    return out[None]


def solution(mesh):
    spec = P(("group", "blk"))
    return jax.shard_map(
        local,
        mesh=mesh,
        in_specs=(P(("group", "blk"), None, None), spec),
        out_specs=P(("group", "blk"), None, None),
        check_vma=False,
    )
```

```python
import jax
import jax.numpy as jnp
import numpy as np
from jax import lax
from jax.experimental import pallas as pl
from jax.experimental.pallas import tpu as pltpu
from jax.sharding import PartitionSpec as P

SIZE = 64
HALF = 32
ROWS = 36
BF = jnp.bfloat16
F32 = jnp.float32


def two_parts(matrix):
    high = np.asarray(matrix, np.float64).astype(BF)
    low = (np.asarray(matrix, np.float64) - high.astype(np.float64)).astype(BF)
    return high, low


def real_basis(points, freqs, period):
    place = np.arange(points)
    rows, marks = [], []
    for freq in freqs:
        waves = [np.cos(2 * np.pi * freq * place / period)]
        waves.append(np.sin(2 * np.pi * freq * place / period))
        for wave in waves:
            norm = np.sqrt(np.sum(wave * wave))
            if norm > 1e-6:
                rows.append(wave / norm)
                marks.append(freq)
    return np.stack(rows), np.asarray(marks, np.float64)


def left_form(matrix):
    high, low = two_parts(matrix)
    return np.concatenate([high, high, low], axis=1)


def right_form(matrix):
    high, low = two_parts(matrix)
    row = np.concatenate([high, low], axis=1)
    return np.concatenate([row, row], axis=0)


def constants():
    full, marks = real_basis(SIZE, range(HALF + 1), SIZE)
    even, even_marks = real_basis(HALF, range(0, HALF + 1, 2), SIZE)
    odd, odd_marks = real_basis(HALF, range(1, HALF, 2), SIZE)
    mix = np.array([[1.0, 1.0], [1.0, -1.0]]) / np.sqrt(2.0)
    lane = np.kron(mix, full)
    mid_marks = np.stack([even_marks, odd_marks], axis=1)
    total = (
        marks[:, None, None, None] ** 2
        + mid_marks[None, :, :, None] ** 2
        + marks[None, None, None, :] ** 2
    )
    step = 2.0 * np.pi / SIZE
    kernel = (np.pi / (step * step * total + 0.25)).astype(np.float32)
    kernel = kernel.reshape(SIZE * HALF, 2 * SIZE)
    parts = (
        left_form(full),
        left_form(full.T),
        right_form(lane.T),
        right_form(lane),
        left_form(np.concatenate([even, odd], axis=0)),
        left_form(np.concatenate([even.T, odd.T], axis=0)),
    )
    table = [np.pad(part, ((0, 0), (0, 256 - part.shape[1]))) for part in parts]
    return np.concatenate(table, axis=0), kernel


WHERE = {
    "fa": (0, 64, 192),
    "ba": (64, 64, 192),
    "fl": (128, 256, 256),
    "bl": (384, 256, 256),
    "fm": (640, 64, 96),
    "bm": (704, 64, 96),
}


def matrix(mats, name):
    start, rows, columns = WHERE[name]
    return mats[0][start : start + rows, :columns]


def split(value):
    high = value.astype(BF)
    low = (value - high.astype(F32)).astype(BF)
    return high, low


def along_rows(matrix, value):
    high, low = split(value)
    stack = jnp.concatenate([high, low, high], axis=0)
    return jnp.dot(matrix, stack, preferred_element_type=F32)


def along_lanes(value, matrix):
    high, low = split(value)
    both = jnp.dot(
        jnp.concatenate([high, low], axis=1), matrix, preferred_element_type=F32
    )
    return both[:, :128] + both[:, 128:]


def to_rows(value):
    count = value.shape[1] // 128
    return jnp.concatenate(
        [value[:, n * 128 : (n + 1) * 128] for n in range(count)], axis=0
    )


def to_lanes(value, rows):
    count = value.shape[0] // rows
    return jnp.concatenate(
        [value[n * rows : (n + 1) * rows] for n in range(count)], axis=1
    )


def pick(value):
    lane = lax.broadcasted_iota(jnp.int32, (HALF, value.shape[1]), 1)
    return jnp.where((lane & 127) < SIZE, value[:HALF], value[HALF:])


def take(refs, lanes):
    parts = [ref[:, lanes] for ref in refs]
    return parts[0] if len(parts) == 1 else jnp.concatenate(parts, axis=0)


def put(refs, lanes, value):
    refs[0][:, lanes] = value[:HALF]
    refs[1][:, lanes] = value[HALF:]


def forward(left, right, mats, area, tiles=16):
    for base in range(0, HALF, tiles):
        lanes = pl.ds(base * 128, tiles * 128)
        value = along_rows(matrix(mats, "fa"), take(left, lanes) * take(right, lanes))
        value = along_lanes(to_rows(value), matrix(mats, "fl"))
        for n in range(tiles):
            area[pl.ds(base + n, SIZE, stride=ROWS), :] = value[n * SIZE : (n + 1) * SIZE]


def middle(mats, area, other, count=32):
    kernel = mats[1]
    for base in range(0, SIZE, count):
        value = jnp.concatenate(
            [area[pl.ds((base + n) * ROWS, HALF), :] for n in range(count)], axis=1
        )
        value = pick(along_rows(matrix(mats, "fm"), value))
        value = value * to_lanes(kernel[pl.ds(base * HALF, count * HALF), :], HALF)
        value = pick(along_rows(matrix(mats, "bm"), value))
        for n in range(count):
            other[pl.ds((base + n) * ROWS, HALF), :] = value[:, n * 128 : (n + 1) * 128]


def backward(mats, other, base, tiles=16):
    value = jnp.concatenate(
        [other[pl.ds(base + n, SIZE, stride=ROWS), :] for n in range(tiles)], axis=0
    )
    value = along_lanes(value, matrix(mats, "bl"))
    return along_rows(matrix(mats, "ba"), to_lanes(value, SIZE))


def pack_body(occ, orb, out, top, bottom):
    scale = jnp.sqrt(jnp.full((1, 128), occ[0], F32))
    low = lax.broadcasted_iota(jnp.int32, (SIZE, 128), 1) < SIZE
    for n in range(HALF // 2):
        first = orb[:, n * 128 : (n + 1) * 128] * scale
        second = orb[:, (n + 16) * 128 : (n + 17) * 128] * scale
        even = jnp.where(low, first, pltpu.roll(second, SIZE, 1))
        odd = jnp.where(low, pltpu.roll(first, SIZE, 1), second)
        for m, value in ((2 * n, even), (2 * n + 1, odd)):
            lanes = slice(m * 128, (m + 1) * 128)
            out[:, lanes] = value
            top[:, lanes] = value[:HALF]
            bottom[:, lanes] = value[HALF:]


def unpack_body(occ, one, two, top, bottom, out):
    scale = -lax.rsqrt(jnp.full((1, 128), occ[0], F32))
    low = lax.broadcasted_iota(jnp.int32, (SIZE, 128), 1) < SIZE
    for n in range(HALF // 2):
        parts = []
        for m in (2 * n, 2 * n + 1):
            lanes = slice(m * 128, (m + 1) * 128)
            three = take((top, bottom), lanes)
            parts.append((one[:, lanes] + two[:, lanes] + three) * scale)
        even, odd = parts
        out[:, n * 128 : (n + 1) * 128] = jnp.where(low, even, pltpu.roll(odd, SIZE, 1))
        out[:, (n + 16) * 128 : (n + 17) * 128] = jnp.where(
            low, pltpu.roll(even, SIZE, 1), odd
        )


WHOLE = jax.ShapeDtypeStruct((SIZE, SIZE * SIZE), F32)
PART = jax.ShapeDtypeStruct((HALF, SIZE * SIZE), F32)
SMEM = pl.BlockSpec(memory_space=pltpu.SMEM)
VMEM = pl.BlockSpec(memory_space=pltpu.VMEM)
COST = 2 * 6 * SIZE**4 * 200
AREA = pltpu.VMEM((SIZE * ROWS, 128), F32)


def call(body, count, outs, scratch=(), work=0, first=VMEM):
    return pl.pallas_call(
        body,
        out_shape=list(outs),
        in_specs=[first] + [VMEM] * (count - 1),
        out_specs=[VMEM] * len(outs),
        scratch_shapes=list(scratch),
        cost_estimate=pl.CostEstimate(
            flops=work * COST, bytes_accessed=1 << 20, transcendentals=0
        ),
        compiler_params=pltpu.CompilerParams(vmem_limit_bytes=20 << 20),
    )


def edge(one, two, mats, areas, finish, tiles=16):
    forward(one, two, mats, areas[0])
    middle(mats, *areas)
    for base in range(0, HALF, tiles):
        value = backward(mats, areas[1], base, tiles)
        lanes = pl.ds(base * 128, tiles * 128)
        finish(lanes, value * take(two, lanes), value * take(one, lanes))


def right_body(home, top, bottom, *rest):
    mats, (home_out, top_out, bottom_out, *area) = rest[:2], rest[2:]

    def finish(lanes, first, second):
        home_out[:, lanes] = first
        put((top_out, bottom_out), lanes, second)

    edge((home,), (top, bottom), mats, area, finish)


def far_body(left, top, bottom, *rest):
    mats, (left_out, top_out, bottom_out, *area) = rest[:2], rest[2:]

    def finish(lanes, first, second):
        left_out[:, lanes] = first
        put((top_out, bottom_out), lanes, second)

    edge((left,), (top, bottom), mats, area, finish)


def left_body(left, home, top, bottom, left_in, home_in, top_in, bottom_in, *rest):
    mats, outs = rest[:2], rest[2:]
    left_out, home_out, top_out, bottom_out, *area = outs

    def finish_home(lanes, first, second):
        left_out[:, lanes] = left_in[:, lanes] + first
        home_out[:, lanes] = home_in[:, lanes] + second

    def finish_right(lanes, first, second):
        left_out[:, lanes] += first
        put((top_out, bottom_out), lanes, take((top_in, bottom_in), lanes) + second)

    edge((left,), (home,), mats, area, finish_home)
    edge((left,), (top, bottom), mats, area, finish_right)


def shift(value, axis, steps):
    count = lax.axis_size(axis)
    pairs = [(source, (source + steps) % count) for source in range(count)]
    return lax.ppermute(value, axis, pairs)


def local(orbitals, occupation):
    mats = [jnp.asarray(item) for item in constants()]
    pair = [WHOLE, PART, PART]
    home, top, bottom = call(pack_body, 2, pair, first=SMEM)(occupation, orbitals[0])
    left = shift(home, "blk", -1)
    right = []
    for part in (top, bottom):
        right.append(shift(part, "blk", 2))
    far = [shift(part, "group", 1) for part in right]
    acc_home, *acc_right = call(right_body, 5, pair, [AREA] * 2, 1)(home, *right, *mats)
    acc_left, *acc_far = call(far_body, 5, pair, [AREA] * 2, 1)(left, *far, *mats)
    from_far = [shift(part, "group", -1) for part in acc_far]
    acc_left, acc_home, *acc_right = call(
        left_body, 10, [WHOLE, WHOLE, PART, PART], [AREA] * 2, 2
    )(left, home, *right, acc_left, acc_home, *acc_right, *mats)
    from_left = shift(acc_left, "blk", 1)
    from_right = [
        shift(one + two, "blk", -2) for one, two in zip(acc_right, from_far)
    ]
    out = call(unpack_body, 5, [WHOLE], first=SMEM)(
        occupation, acc_home, from_left, *from_right
    )[0]
    return out[None]


def solution(mesh):
    spec = P(("group", "blk"))
    return jax.shard_map(
        local,
        mesh=mesh,
        in_specs=(P(("group", "blk"), None, None), spec),
        out_specs=P(("group", "blk"), None, None),
        check_vma=False,
    )
```

```python
import jax
import jax.numpy as jnp
import numpy as np
from jax import lax
from jax.experimental import pallas as pl
from jax.experimental.pallas import tpu as pltpu
from jax.sharding import PartitionSpec as P

SIZE = 64
HALF = 32
ROWS = 36
BF = jnp.bfloat16
F32 = jnp.float32


def two_parts(matrix):
    high = np.asarray(matrix, np.float64).astype(BF)
    low = (np.asarray(matrix, np.float64) - high.astype(np.float64)).astype(BF)
    return high, low


def real_basis(points, freqs, period):
    place = np.arange(points)
    rows, marks = [], []
    for freq in freqs:
        waves = [np.cos(2 * np.pi * freq * place / period)]
        waves.append(np.sin(2 * np.pi * freq * place / period))
        for wave in waves:
            norm = np.sqrt(np.sum(wave * wave))
            if norm > 1e-6:
                rows.append(wave / norm)
                marks.append(freq)
    return np.stack(rows), np.asarray(marks, np.float64)


def left_form(matrix):
    high, low = two_parts(matrix)
    return np.concatenate([high, high, low], axis=1)


def right_form(matrix):
    high, low = two_parts(matrix)
    row = np.concatenate([high, low], axis=1)
    return np.concatenate([row, row], axis=0)


def constants():
    full, marks = real_basis(SIZE, range(HALF + 1), SIZE)
    even, even_marks = real_basis(HALF, range(0, HALF + 1, 2), SIZE)
    odd, odd_marks = real_basis(HALF, range(1, HALF, 2), SIZE)
    mix = np.array([[1.0, 1.0], [1.0, -1.0]]) / np.sqrt(2.0)
    lane = np.kron(mix, full)
    mid_marks = np.stack([even_marks, odd_marks], axis=1)
    total = (
        marks[:, None, None, None] ** 2
        + mid_marks[None, :, :, None] ** 2
        + marks[None, None, None, :] ** 2
    )
    step = 2.0 * np.pi / SIZE
    kernel = (np.pi / (step * step * total + 0.25)).astype(np.float32)
    kernel = kernel.reshape(SIZE * HALF, 2 * SIZE)
    parts = (
        left_form(full),
        left_form(full.T),
        right_form(lane.T),
        right_form(lane),
        left_form(np.concatenate([even, odd], axis=0)),
        left_form(np.concatenate([even.T, odd.T], axis=0)),
    )
    table = [np.pad(part, ((0, 0), (0, 256 - part.shape[1]))) for part in parts]
    return np.concatenate(table, axis=0), kernel


WHERE = {
    "fa": (0, 64, 192),
    "ba": (64, 64, 192),
    "fl": (128, 256, 256),
    "bl": (384, 256, 256),
    "fm": (640, 64, 96),
    "bm": (704, 64, 96),
}


def matrix(mats, name):
    start, rows, columns = WHERE[name]
    return mats[0][start : start + rows, :columns]


def split(value):
    high = value.astype(BF)
    low = (value - high.astype(F32)).astype(BF)
    return high, low


def along_rows(matrix, value):
    high, low = split(value)
    stack = jnp.concatenate([high, low, high], axis=0)
    return jnp.dot(matrix, stack, preferred_element_type=F32)


def along_lanes(value, matrix):
    high, low = split(value)
    both = jnp.dot(
        jnp.concatenate([high, low], axis=1), matrix, preferred_element_type=F32
    )
    return both[:, :128] + both[:, 128:]


def to_rows(value):
    count = value.shape[1] // 128
    return jnp.concatenate(
        [value[:, n * 128 : (n + 1) * 128] for n in range(count)], axis=0
    )


def to_lanes(value, rows):
    count = value.shape[0] // rows
    return jnp.concatenate(
        [value[n * rows : (n + 1) * rows] for n in range(count)], axis=1
    )


def pick(value):
    lane = lax.broadcasted_iota(jnp.int32, (HALF, value.shape[1]), 1)
    return jnp.where((lane & 127) < SIZE, value[:HALF], value[HALF:])


def take(refs, lanes):
    parts = [ref[:, lanes] for ref in refs]
    return parts[0] if len(parts) == 1 else jnp.concatenate(parts, axis=0)


def put(refs, lanes, value):
    refs[0][:, lanes] = value[:HALF]
    refs[1][:, lanes] = value[HALF:]


def forward(left, right, mats, area, tiles=16):
    for base in range(0, HALF, tiles):
        lanes = pl.ds(base * 128, tiles * 128)
        value = along_rows(matrix(mats, "fa"), take(left, lanes) * take(right, lanes))
        value = along_lanes(to_rows(value), matrix(mats, "fl"))
        for n in range(tiles):
            area[pl.ds(base + n, SIZE, stride=ROWS), :] = value[n * SIZE : (n + 1) * SIZE]


def middle(mats, area, other, count=32):
    kernel = mats[1]
    for base in range(0, SIZE, count):
        value = jnp.concatenate(
            [area[pl.ds((base + n) * ROWS, HALF), :] for n in range(count)], axis=1
        )
        value = pick(along_rows(matrix(mats, "fm"), value))
        value = value * to_lanes(kernel[pl.ds(base * HALF, count * HALF), :], HALF)
        value = pick(along_rows(matrix(mats, "bm"), value))
        for n in range(count):
            other[pl.ds((base + n) * ROWS, HALF), :] = value[:, n * 128 : (n + 1) * 128]


def backward(mats, other, base, tiles=16):
    value = jnp.concatenate(
        [other[pl.ds(base + n, SIZE, stride=ROWS), :] for n in range(tiles)], axis=0
    )
    value = along_lanes(value, matrix(mats, "bl"))
    return along_rows(matrix(mats, "ba"), to_lanes(value, SIZE))


def pack_body(occ, orb, out, top, bottom):
    scale = jnp.sqrt(jnp.full((1, 128), occ[0], F32))
    low = lax.broadcasted_iota(jnp.int32, (SIZE, 128), 1) < SIZE
    for n in range(HALF // 2):
        first = orb[:, n * 128 : (n + 1) * 128] * scale
        second = orb[:, (n + 16) * 128 : (n + 17) * 128] * scale
        even = jnp.where(low, first, pltpu.roll(second, SIZE, 1))
        odd = jnp.where(low, pltpu.roll(first, SIZE, 1), second)
        for m, value in ((2 * n, even), (2 * n + 1, odd)):
            lanes = slice(m * 128, (m + 1) * 128)
            out[:, lanes] = value
            top[:, lanes] = value[:HALF]
            bottom[:, lanes] = value[HALF:]


def unpack_body(occ, one, two, top, bottom, out):
    scale = -lax.rsqrt(jnp.full((1, 128), occ[0], F32))
    low = lax.broadcasted_iota(jnp.int32, (SIZE, 128), 1) < SIZE
    for n in range(HALF // 2):
        parts = []
        for m in (2 * n, 2 * n + 1):
            lanes = slice(m * 128, (m + 1) * 128)
            three = take((top, bottom), lanes)
            parts.append((one[:, lanes] + two[:, lanes] + three) * scale)
        even, odd = parts
        out[:, n * 128 : (n + 1) * 128] = jnp.where(low, even, pltpu.roll(odd, SIZE, 1))
        out[:, (n + 16) * 128 : (n + 17) * 128] = jnp.where(
            low, pltpu.roll(even, SIZE, 1), odd
        )


WHOLE = jax.ShapeDtypeStruct((SIZE, SIZE * SIZE), F32)
PART = jax.ShapeDtypeStruct((HALF, SIZE * SIZE), F32)
SMEM = pl.BlockSpec(memory_space=pltpu.SMEM)
VMEM = pl.BlockSpec(memory_space=pltpu.VMEM)
COST = 2 * 6 * SIZE**4 * 200
AREA = pltpu.VMEM((SIZE * ROWS, 128), F32)


def call(body, count, outs, scratch=(), work=0, first=VMEM):
    return pl.pallas_call(
        body,
        out_shape=list(outs),
        in_specs=[first] + [VMEM] * (count - 1),
        out_specs=[VMEM] * len(outs),
        scratch_shapes=list(scratch),
        cost_estimate=pl.CostEstimate(
            flops=work * COST, bytes_accessed=1 << 20, transcendentals=0
        ),
        compiler_params=pltpu.CompilerParams(vmem_limit_bytes=20 << 20),
    )


def edge(one, two, mats, areas, finish, tiles=16):
    forward(one, two, mats, areas[0])
    middle(mats, *areas)
    for base in range(0, HALF, tiles):
        value = backward(mats, areas[1], base, tiles)
        lanes = pl.ds(base * 128, tiles * 128)
        finish(lanes, value * take(two, lanes), value * take(one, lanes))


def first_body(home, right, near_top, near_bottom, *rest):
    mats, outs = rest[:2], rest[2:]
    home_out, right_out, top_out, bottom_out, *areas = outs

    def finish_home(lanes, first, second):
        home_out[:, lanes] = first
        right_out[:, lanes] = second

    def finish_near(lanes, first, second):
        right_out[:, lanes] += second
        put((top_out, bottom_out), lanes, first)

    edge((home,), (right,), mats, areas, finish_home)
    edge((near_top, near_bottom), (right,), mats, areas, finish_near)


def second_body(left_top, left_bottom, home, right, far, home_in, right_in, *rest):
    mats, outs = rest[:2], rest[2:]
    top_out, bottom_out, home_out, right_out, far_out, *areas = outs
    left, left_outs = (left_top, left_bottom), (top_out, bottom_out)

    def finish_far(lanes, first, second):
        put(left_outs, lanes, first)
        far_out[:, lanes] = second

    def finish_right(lanes, first, second):
        put(left_outs, lanes, take(left_outs, lanes) + first)
        right_out[:, lanes] = right_in[:, lanes] + second

    def finish_home(lanes, first, second):
        put(left_outs, lanes, take(left_outs, lanes) + first)
        home_out[:, lanes] = home_in[:, lanes] + second

    edge(left, (far,), mats, areas, finish_far)
    edge(left, (right,), mats, areas, finish_right)
    edge(left, (home,), mats, areas, finish_home)


AXES = ("group", "blk")


def send(value, pairs):
    return lax.ppermute(value, AXES, pairs)


def routes(groups, blocks):
    def at(group, place):
        return (group % groups) * blocks + place % blocks

    outward, inward, across = [], [], []
    for group in range(groups):
        for place in range(blocks):
            source, target = at(group, place + 1), at(group, place)
            if group % 2:
                relay = at(group + 1, place + 1)
                across.append((at(group - 1, place), target))
            else:
                relay = at(group - 1, place)
            outward.append((source, relay))
            inward.append((relay, target))
    behind = [
        (at(group, place - 2), at(group, place))
        for group in range(groups)
        for place in range(blocks)
    ]
    return outward, inward, across, behind


def turned(pairs):
    return [(target, source) for source, target in pairs]


def local(orbitals, occupation):
    mats = [jnp.asarray(item) for item in constants()]
    groups, blocks = lax.axis_size("group"), lax.axis_size("blk")
    outward, inward, across, behind = routes(groups, blocks)
    odd = lax.axis_index("group") % 2 == 1
    home, top, bottom = call(pack_body, 2, [WHOLE, PART, PART], first=SMEM)(
        occupation, orbitals[0]
    )
    right = send(home, behind)
    near = [send(top, outward), send(bottom, outward)]
    left = [send(near[0], inward), send(near[1], inward)]
    far = send(right, across)
    near = [jnp.where(odd, part, 0.0) for part in near]
    acc_home, acc_right, *acc_near = call(
        first_body, 6, [WHOLE, WHOLE, PART, PART], [AREA] * 2, 2
    )(home, right, *near, *mats)
    *acc_left, acc_home, acc_right, acc_far = call(
        second_body, 9, [PART, PART, WHOLE, WHOLE, WHOLE], [AREA] * 2, 3
    )(*left, home, right, far, acc_home, acc_right, *mats)
    back = [send(acc_left[0], turned(inward)), send(acc_left[1], turned(inward))]
    from_far = send(acc_far, turned(across))
    from_right = send(acc_right + from_far, turned(behind))
    from_left = [
        send(back[0] + acc_near[0], turned(outward)),
        send(back[1] + acc_near[1], turned(outward)),
    ]
    out = call(unpack_body, 5, [WHOLE], first=SMEM)(
        occupation, acc_home, from_right, *from_left
    )[0]
    return out[None]


def solution(mesh):
    spec = P(("group", "blk"))
    return jax.shard_map(
        local,
        mesh=mesh,
        in_specs=(P(("group", "blk"), None, None), spec),
        out_specs=P(("group", "blk"), None, None),
        check_vma=False,
    )
```

```python
import jax
import jax.numpy as jnp
import numpy as np
from jax import lax
from jax.experimental import pallas as pl
from jax.experimental.pallas import tpu as pltpu
from jax.sharding import PartitionSpec as P

SIZE = 64
HALF = 32
ROWS = 36
BF = jnp.bfloat16
F32 = jnp.float32


def two_parts(matrix):
    high = np.asarray(matrix, np.float64).astype(BF)
    low = (np.asarray(matrix, np.float64) - high.astype(np.float64)).astype(BF)
    return high, low


def real_basis(points, freqs, period):
    place = np.arange(points)
    rows, marks = [], []
    for freq in freqs:
        waves = [np.cos(2 * np.pi * freq * place / period)]
        waves.append(np.sin(2 * np.pi * freq * place / period))
        for wave in waves:
            norm = np.sqrt(np.sum(wave * wave))
            if norm > 1e-6:
                rows.append(wave / norm)
                marks.append(freq)
    return np.stack(rows), np.asarray(marks, np.float64)


def left_form(matrix):
    high, low = two_parts(matrix)
    return np.concatenate([high, high, low], axis=1)


def right_form(matrix):
    high, low = two_parts(matrix)
    row = np.concatenate([high, low], axis=1)
    return np.concatenate([row, row], axis=0)


def constants():
    full, marks = real_basis(SIZE, range(HALF + 1), SIZE)
    even, even_marks = real_basis(HALF, range(0, HALF + 1, 2), SIZE)
    odd, odd_marks = real_basis(HALF, range(1, HALF, 2), SIZE)
    mix = np.array([[1.0, 1.0], [1.0, -1.0]]) / np.sqrt(2.0)
    lane = np.kron(mix, full)
    mid_marks = np.stack([even_marks, odd_marks], axis=1)
    total = (
        marks[:, None, None, None] ** 2
        + mid_marks[None, :, :, None] ** 2
        + marks[None, None, None, :] ** 2
    )
    step = 2.0 * np.pi / SIZE
    kernel = (np.pi / (step * step * total + 0.25)).astype(np.float32)
    kernel = kernel.reshape(SIZE * HALF, 2 * SIZE)
    parts = (
        left_form(full),
        left_form(full.T),
        right_form(lane.T),
        right_form(lane),
        left_form(np.concatenate([even, odd], axis=0)),
        left_form(np.concatenate([even.T, odd.T], axis=0)),
    )
    table = [np.pad(part, ((0, 0), (0, 256 - part.shape[1]))) for part in parts]
    return np.concatenate(table, axis=0), kernel


WHERE = {
    "fa": (0, 64, 192),
    "ba": (64, 64, 192),
    "fl": (128, 256, 256),
    "bl": (384, 256, 256),
    "fm": (640, 64, 96),
    "bm": (704, 64, 96),
}


def matrix(mats, name):
    start, rows, columns = WHERE[name]
    return mats[0][start : start + rows, :columns]


def split(value):
    high = value.astype(BF)
    low = (value - high.astype(F32)).astype(BF)
    return high, low


def along_rows(matrix, value):
    high, low = split(value)
    stack = jnp.concatenate([high, low, high], axis=0)
    return jnp.dot(matrix, stack, preferred_element_type=F32)


def along_lanes(value, matrix):
    high, low = split(value)
    both = jnp.dot(
        jnp.concatenate([high, low], axis=1), matrix, preferred_element_type=F32
    )
    return both[:, :128] + both[:, 128:]


def to_rows(value):
    count = value.shape[1] // 128
    return jnp.concatenate(
        [value[:, n * 128 : (n + 1) * 128] for n in range(count)], axis=0
    )


def to_lanes(value, rows):
    count = value.shape[0] // rows
    return jnp.concatenate(
        [value[n * rows : (n + 1) * rows] for n in range(count)], axis=1
    )


def pick(value):
    lane = lax.broadcasted_iota(jnp.int32, (HALF, value.shape[1]), 1)
    return jnp.where((lane & 127) < SIZE, value[:HALF], value[HALF:])


def take(refs, lanes):
    parts = [ref[:, lanes] for ref in refs]
    return parts[0] if len(parts) == 1 else jnp.concatenate(parts, axis=0)


def put(refs, lanes, value):
    refs[0][:, lanes] = value[:HALF]
    refs[1][:, lanes] = value[HALF:]


def forward(left, right, mats, area, tiles=16):
    for base in range(0, HALF, tiles):
        lanes = pl.ds(base * 128, tiles * 128)
        value = along_rows(matrix(mats, "fa"), take(left, lanes) * take(right, lanes))
        value = along_lanes(to_rows(value), matrix(mats, "fl"))
        for n in range(tiles):
            area[pl.ds(base + n, SIZE, stride=ROWS), :] = value[n * SIZE : (n + 1) * SIZE]


def middle(mats, area, other, count=32):
    kernel = mats[1]
    for base in range(0, SIZE, count):
        value = jnp.concatenate(
            [area[pl.ds((base + n) * ROWS, HALF), :] for n in range(count)], axis=1
        )
        value = pick(along_rows(matrix(mats, "fm"), value))
        value = value * to_lanes(kernel[pl.ds(base * HALF, count * HALF), :], HALF)
        value = pick(along_rows(matrix(mats, "bm"), value))
        for n in range(count):
            other[pl.ds((base + n) * ROWS, HALF), :] = value[:, n * 128 : (n + 1) * 128]


def backward(mats, other, base, tiles=16):
    value = jnp.concatenate(
        [other[pl.ds(base + n, SIZE, stride=ROWS), :] for n in range(tiles)], axis=0
    )
    value = along_lanes(value, matrix(mats, "bl"))
    return along_rows(matrix(mats, "ba"), to_lanes(value, SIZE))


def pack_body(occ, orb, out, top, bottom):
    scale = jnp.sqrt(jnp.full((1, 128), occ[0], F32))
    low = lax.broadcasted_iota(jnp.int32, (SIZE, 128), 1) < SIZE
    for n in range(HALF // 2):
        first = orb[:, n * 128 : (n + 1) * 128] * scale
        second = orb[:, (n + 16) * 128 : (n + 17) * 128] * scale
        even = jnp.where(low, first, pltpu.roll(second, SIZE, 1))
        odd = jnp.where(low, pltpu.roll(first, SIZE, 1), second)
        for m, value in ((2 * n, even), (2 * n + 1, odd)):
            lanes = slice(m * 128, (m + 1) * 128)
            out[:, lanes] = value
            top[:, lanes] = value[:HALF]
            bottom[:, lanes] = value[HALF:]


def unpack_body(occ, one, two, top, bottom, out):
    scale = -lax.rsqrt(jnp.full((1, 128), occ[0], F32))
    low = lax.broadcasted_iota(jnp.int32, (SIZE, 128), 1) < SIZE
    for n in range(HALF // 2):
        parts = []
        for m in (2 * n, 2 * n + 1):
            lanes = slice(m * 128, (m + 1) * 128)
            three = take((top, bottom), lanes)
            parts.append((one[:, lanes] + two[:, lanes] + three) * scale)
        even, odd = parts
        out[:, n * 128 : (n + 1) * 128] = jnp.where(low, even, pltpu.roll(odd, SIZE, 1))
        out[:, (n + 16) * 128 : (n + 17) * 128] = jnp.where(
            low, pltpu.roll(even, SIZE, 1), odd
        )


WHOLE = jax.ShapeDtypeStruct((SIZE, SIZE * SIZE), F32)
PART = jax.ShapeDtypeStruct((HALF, SIZE * SIZE), F32)
SMEM = pl.BlockSpec(memory_space=pltpu.SMEM)
VMEM = pl.BlockSpec(memory_space=pltpu.VMEM)
COST = 2 * 6 * SIZE**4 * 200
AREA = pltpu.VMEM((SIZE * ROWS, 128), F32)


def call(body, count, outs, scratch=(), work=0, first=VMEM):
    return pl.pallas_call(
        body,
        out_shape=list(outs),
        in_specs=[first] + [VMEM] * (count - 1),
        out_specs=[VMEM] * len(outs),
        scratch_shapes=list(scratch),
        cost_estimate=pl.CostEstimate(
            flops=work * COST, bytes_accessed=1 << 20, transcendentals=0
        ),
        compiler_params=pltpu.CompilerParams(vmem_limit_bytes=20 << 20),
    )


def edge(one, two, mats, areas, finish, tiles=16):
    forward(one, two, mats, areas[0])
    middle(mats, *areas)
    for base in range(0, HALF, tiles):
        value = backward(mats, areas[1], base, tiles)
        lanes = pl.ds(base * 128, tiles * 128)
        finish(lanes, value * take(two, lanes), value * take(one, lanes))


def first_body(home, right, near_top, near_bottom, *rest):
    mats, outs = rest[:2], rest[2:]
    home_out, right_out, top_out, bottom_out, *areas = outs

    def finish_home(lanes, first, second):
        home_out[:, lanes] = first
        right_out[:, lanes] = second

    def finish_near(lanes, first, second):
        right_out[:, lanes] += second
        put((top_out, bottom_out), lanes, first)

    edge((home,), (right,), mats, areas, finish_home)
    edge((near_top, near_bottom), (right,), mats, areas, finish_near)


def far_body(left_top, left_bottom, far, *rest):
    mats, (top_out, bottom_out, far_out, *areas) = rest[:2], rest[2:]

    def finish(lanes, first, second):
        put((top_out, bottom_out), lanes, first)
        far_out[:, lanes] = second

    edge((left_top, left_bottom), (far,), mats, areas, finish)


def second_body(left_top, left_bottom, home, right, top_in, bottom_in, home_in, right_in, *rest):
    mats, outs = rest[:2], rest[2:]
    top_out, bottom_out, home_out, right_out, *areas = outs
    left, left_outs = (left_top, left_bottom), (top_out, bottom_out)

    def finish_right(lanes, first, second):
        put(left_outs, lanes, take((top_in, bottom_in), lanes) + first)
        right_out[:, lanes] = right_in[:, lanes] + second

    def finish_home(lanes, first, second):
        put(left_outs, lanes, take(left_outs, lanes) + first)
        home_out[:, lanes] = home_in[:, lanes] + second

    edge(left, (right,), mats, areas, finish_right)
    edge(left, (home,), mats, areas, finish_home)


AXES = ("group", "blk")


def send(value, pairs):
    return lax.ppermute(value, AXES, pairs)


def routes(groups, blocks):
    def at(group, place):
        return (group % groups) * blocks + place % blocks

    outward, inward, across = [], [], []
    for group in range(groups):
        for place in range(blocks):
            source, target = at(group, place + 1), at(group, place)
            if group % 2:
                relay = at(group + 1, place + 1)
                across.append((at(group - 1, place), target))
            else:
                relay = at(group - 1, place)
            outward.append((source, relay))
            inward.append((relay, target))
    behind = [
        (at(group, place - 2), at(group, place))
        for group in range(groups)
        for place in range(blocks)
    ]
    return outward, inward, across, behind


def turned(pairs):
    return [(target, source) for source, target in pairs]


def local(orbitals, occupation):
    mats = [jnp.asarray(item) for item in constants()]
    groups, blocks = lax.axis_size("group"), lax.axis_size("blk")
    outward, inward, across, behind = routes(groups, blocks)
    odd = lax.axis_index("group") % 2 == 1
    home, top, bottom = call(pack_body, 2, [WHOLE, PART, PART], first=SMEM)(
        occupation, orbitals[0]
    )
    right = send(home, behind)
    near = [send(top, outward), send(bottom, outward)]
    left = [send(near[0], inward), send(near[1], inward)]
    far = send(right, across)
    near = [jnp.where(odd, part, 0.0) for part in near]
    acc_home, acc_right, *acc_near = call(
        first_body, 6, [WHOLE, WHOLE, PART, PART], [AREA] * 2, 2
    )(home, right, *near, *mats)
    *acc_left, acc_far = call(far_body, 5, [PART, PART, WHOLE], [AREA] * 2, 1)(
        *left, far, *mats
    )
    from_far = send(acc_far, turned(across))
    *acc_left, acc_home, acc_right = call(
        second_body, 10, [PART, PART, WHOLE, WHOLE], [AREA] * 2, 2
    )(*left, home, right, *acc_left, acc_home, acc_right, *mats)
    back = [send(acc_left[0], turned(inward)), send(acc_left[1], turned(inward))]
    from_right = send(acc_right + from_far, turned(behind))
    from_left = [
        send(back[0] + acc_near[0], turned(outward)),
        send(back[1] + acc_near[1], turned(outward)),
    ]
    out = call(unpack_body, 5, [WHOLE], first=SMEM)(
        occupation, acc_home, from_right, *from_left
    )[0]
    return out[None]


def solution(mesh):
    spec = P(("group", "blk"))
    return jax.shard_map(
        local,
        mesh=mesh,
        in_specs=(P(("group", "blk"), None, None), spec),
        out_specs=P(("group", "blk"), None, None),
        check_vma=False,
    )
```

```python
import jax
import jax.numpy as jnp
import numpy as np
from jax import lax
from jax.experimental import pallas as pl
from jax.experimental.pallas import tpu as pltpu
from jax.sharding import PartitionSpec as P

SIZE = 64
HALF = 32
ROWS = 36
BF = jnp.bfloat16
F32 = jnp.float32


def two_parts(matrix):
    high = np.asarray(matrix, np.float64).astype(BF)
    low = (np.asarray(matrix, np.float64) - high.astype(np.float64)).astype(BF)
    return high, low


def real_basis(points, freqs, period):
    place = np.arange(points)
    rows, marks = [], []
    for freq in freqs:
        waves = [np.cos(2 * np.pi * freq * place / period)]
        waves.append(np.sin(2 * np.pi * freq * place / period))
        for wave in waves:
            norm = np.sqrt(np.sum(wave * wave))
            if norm > 1e-6:
                rows.append(wave / norm)
                marks.append(freq)
    return np.stack(rows), np.asarray(marks, np.float64)


def left_form(matrix):
    high, low = two_parts(matrix)
    return np.concatenate([high, high, low], axis=1)


def right_form(matrix):
    high, low = two_parts(matrix)
    row = np.concatenate([high, low], axis=1)
    return np.concatenate([row, row], axis=0)


def constants():
    full, marks = real_basis(SIZE, range(HALF + 1), SIZE)
    even, even_marks = real_basis(HALF, range(0, HALF + 1, 2), SIZE)
    odd, odd_marks = real_basis(HALF, range(1, HALF, 2), SIZE)
    mix = np.array([[1.0, 1.0], [1.0, -1.0]]) / np.sqrt(2.0)
    lane = np.kron(mix, full)
    mid_marks = np.stack([even_marks, odd_marks], axis=1)
    total = (
        marks[:, None, None, None] ** 2
        + mid_marks[None, :, :, None] ** 2
        + marks[None, None, None, :] ** 2
    )
    step = 2.0 * np.pi / SIZE
    kernel = (np.pi / (step * step * total + 0.25)).astype(np.float32)
    kernel = kernel.reshape(SIZE * HALF, 2 * SIZE)
    parts = (
        left_form(full),
        left_form(full.T),
        right_form(lane.T),
        right_form(lane),
        left_form(np.concatenate([even, odd], axis=0)),
        left_form(np.concatenate([even.T, odd.T], axis=0)),
    )
    table = [np.pad(part, ((0, 0), (0, 256 - part.shape[1]))) for part in parts]
    return np.concatenate(table, axis=0), kernel


WHERE = {
    "fa": (0, 64, 192),
    "ba": (64, 64, 192),
    "fl": (128, 256, 256),
    "bl": (384, 256, 256),
    "fm": (640, 64, 96),
    "bm": (704, 64, 96),
}


def matrix(mats, name):
    start, rows, columns = WHERE[name]
    return mats[0][start : start + rows, :columns]


def split(value):
    high = value.astype(BF)
    low = (value - high.astype(F32)).astype(BF)
    return high, low


def along_rows(matrix, value):
    high, low = split(value)
    stack = jnp.concatenate([high, low, high], axis=0)
    return jnp.dot(matrix, stack, preferred_element_type=F32)


def along_lanes(value, matrix):
    high, low = split(value)
    both = jnp.dot(
        jnp.concatenate([high, low], axis=1), matrix, preferred_element_type=F32
    )
    return both[:, :128] + both[:, 128:]


def to_rows(value):
    count = value.shape[1] // 128
    return jnp.concatenate(
        [value[:, n * 128 : (n + 1) * 128] for n in range(count)], axis=0
    )


def to_lanes(value, rows):
    count = value.shape[0] // rows
    return jnp.concatenate(
        [value[n * rows : (n + 1) * rows] for n in range(count)], axis=1
    )


def pick(value):
    lane = lax.broadcasted_iota(jnp.int32, (HALF, value.shape[1]), 1)
    return jnp.where((lane & 127) < SIZE, value[:HALF], value[HALF:])


def take(refs, lanes):
    parts = [ref[:, lanes] for ref in refs]
    return parts[0] if len(parts) == 1 else jnp.concatenate(parts, axis=0)


def put(refs, lanes, value):
    refs[0][:, lanes] = value[:HALF]
    refs[1][:, lanes] = value[HALF:]


def forward(left, right, mats, area, tiles=16):
    for base in range(0, HALF, tiles):
        lanes = pl.ds(base * 128, tiles * 128)
        value = along_rows(matrix(mats, "fa"), take(left, lanes) * take(right, lanes))
        value = along_lanes(to_rows(value), matrix(mats, "fl"))
        for n in range(tiles):
            area[pl.ds(base + n, SIZE, stride=ROWS), :] = value[n * SIZE : (n + 1) * SIZE]


def middle(mats, area, other, count=32):
    kernel = mats[1]
    for base in range(0, SIZE, count):
        value = jnp.concatenate(
            [area[pl.ds((base + n) * ROWS, HALF), :] for n in range(count)], axis=1
        )
        value = pick(along_rows(matrix(mats, "fm"), value))
        value = value * to_lanes(kernel[pl.ds(base * HALF, count * HALF), :], HALF)
        value = pick(along_rows(matrix(mats, "bm"), value))
        for n in range(count):
            other[pl.ds((base + n) * ROWS, HALF), :] = value[:, n * 128 : (n + 1) * 128]


def backward(mats, other, base, tiles=16):
    value = jnp.concatenate(
        [other[pl.ds(base + n, SIZE, stride=ROWS), :] for n in range(tiles)], axis=0
    )
    value = along_lanes(value, matrix(mats, "bl"))
    return along_rows(matrix(mats, "ba"), to_lanes(value, SIZE))


def pack_body(occ, orb, out, top, bottom):
    scale = jnp.sqrt(jnp.full((1, 128), occ[0], F32))
    low = lax.broadcasted_iota(jnp.int32, (SIZE, 128), 1) < SIZE
    for n in range(HALF // 2):
        first = orb[:, n * 128 : (n + 1) * 128] * scale
        second = orb[:, (n + 16) * 128 : (n + 17) * 128] * scale
        even = jnp.where(low, first, pltpu.roll(second, SIZE, 1))
        odd = jnp.where(low, pltpu.roll(first, SIZE, 1), second)
        for m, value in ((2 * n, even), (2 * n + 1, odd)):
            lanes = slice(m * 128, (m + 1) * 128)
            out[:, lanes] = value
            top[:, lanes] = value[:HALF]
            bottom[:, lanes] = value[HALF:]


def unpack_body(occ, one, two, whole, top, bottom, out):
    scale = -lax.rsqrt(jnp.full((1, 128), occ[0], F32))
    low = lax.broadcasted_iota(jnp.int32, (SIZE, 128), 1) < SIZE
    for n in range(HALF // 2):
        parts = []
        for m in (2 * n, 2 * n + 1):
            lanes = slice(m * 128, (m + 1) * 128)
            three = whole[:, lanes] + take((top, bottom), lanes)
            parts.append((one[:, lanes] + two[:, lanes] + three) * scale)
        even, odd = parts
        out[:, n * 128 : (n + 1) * 128] = jnp.where(low, even, pltpu.roll(odd, SIZE, 1))
        out[:, (n + 16) * 128 : (n + 17) * 128] = jnp.where(
            low, pltpu.roll(even, SIZE, 1), odd
        )


WHOLE = jax.ShapeDtypeStruct((SIZE, SIZE * SIZE), F32)
PART = jax.ShapeDtypeStruct((HALF, SIZE * SIZE), F32)
SMEM = pl.BlockSpec(memory_space=pltpu.SMEM)
VMEM = pl.BlockSpec(memory_space=pltpu.VMEM)
COST = 2 * 6 * SIZE**4 * 200
AREA = pltpu.VMEM((SIZE * ROWS, 128), F32)


def call(body, count, outs, scratch=(), work=0, first=VMEM):
    return pl.pallas_call(
        body,
        out_shape=list(outs),
        in_specs=[first] + [VMEM] * (count - 1),
        out_specs=[VMEM] * len(outs),
        scratch_shapes=list(scratch),
        cost_estimate=pl.CostEstimate(
            flops=work * COST, bytes_accessed=1 << 20, transcendentals=0
        ),
        compiler_params=pltpu.CompilerParams(vmem_limit_bytes=20 << 20),
    )


def edge(one, two, mats, areas, finish, tiles=16):
    forward(one, two, mats, areas[0])
    middle(mats, *areas)
    for base in range(0, HALF, tiles):
        value = backward(mats, areas[1], base, tiles)
        lanes = pl.ds(base * 128, tiles * 128)
        finish(lanes, value * take(two, lanes), value * take(one, lanes))


def first_body(home, right, near_top, near_bottom, *rest):
    mats, outs = rest[:2], rest[2:]
    home_out, right_out, top_out, bottom_out, *areas = outs

    def finish_home(lanes, first, second):
        home_out[:, lanes] = first
        right_out[:, lanes] = second

    def finish_near(lanes, first, second):
        right_out[:, lanes] += second
        put((top_out, bottom_out), lanes, first)

    edge((home,), (right,), mats, areas, finish_home)
    edge((near_top, near_bottom), (right,), mats, areas, finish_near)


def far_body(left_top, left_bottom, far, *rest):
    mats, (top_out, bottom_out, far_out, *areas) = rest[:2], rest[2:]

    def finish(lanes, first, second):
        put((top_out, bottom_out), lanes, first)
        far_out[:, lanes] = second

    edge((left_top, left_bottom), (far,), mats, areas, finish)


def second_body(left_top, left_bottom, home, right, top_in, bottom_in, home_in, right_in, *rest):
    mats, outs = rest[:2], rest[2:]
    whole_out, top_out, bottom_out, home_out, right_out, *areas = outs
    left, left_outs = (left_top, left_bottom), (top_out, bottom_out)

    def finish_right(lanes, first, second):
        put(left_outs, lanes, take((top_in, bottom_in), lanes) + first)
        right_out[:, lanes] = right_in[:, lanes] + second

    def finish_home(lanes, first, second):
        total = take(left_outs, lanes) + first
        put(left_outs, lanes, total)
        whole_out[:, lanes] = total
        home_out[:, lanes] = home_in[:, lanes] + second

    edge(left, (right,), mats, areas, finish_right)
    edge(left, (home,), mats, areas, finish_home)


AXES = ("group", "blk")


def send(value, pairs):
    return lax.ppermute(value, AXES, pairs)


def routes(groups, blocks):
    def at(group, place):
        return (group % groups) * blocks + place % blocks

    outward, inward, direct, across, behind = [], [], [], [], []
    for group in range(groups):
        for place in range(blocks):
            source, target = at(group, place + 1), at(group, place)
            relay = at(group - 1, place)
            if group % 2:
                direct.append((source, target))
                across.append((relay, target))
            else:
                outward.append((source, relay))
                inward.append((relay, target))
            behind.append((at(group, place - 2), target))
    return outward, inward, direct, across, behind


def turned(pairs):
    return [(target, source) for source, target in pairs]


def local(orbitals, occupation):
    mats = [jnp.asarray(item) for item in constants()]
    groups, blocks = lax.axis_size("group"), lax.axis_size("blk")
    outward, inward, direct, across, behind = routes(groups, blocks)
    home, top, bottom = call(pack_body, 2, [WHOLE, PART, PART], first=SMEM)(
        occupation, orbitals[0]
    )
    right = send(home, behind)
    near = [send(top, outward), send(bottom, outward)]
    whole = send(home, direct)
    left = [send(near[0], inward), send(near[1], inward)]
    left = [left[0] + whole[:HALF], left[1] + whole[HALF:]]
    far = send(right, across)
    acc_home, acc_right, *acc_near = call(
        first_body, 6, [WHOLE, WHOLE, PART, PART], [AREA] * 2, 2
    )(home, right, *near, *mats)
    *acc_left, acc_far = call(far_body, 5, [PART, PART, WHOLE], [AREA] * 2, 1)(
        *left, far, *mats
    )
    from_far = send(acc_far, turned(across))
    acc_whole, *acc_left, acc_home, acc_right = call(
        second_body, 10, [WHOLE, PART, PART, WHOLE, WHOLE], [AREA] * 2, 2
    )(*left, home, right, *acc_left, acc_home, acc_right, *mats)
    back = [send(acc_left[0], turned(inward)), send(acc_left[1], turned(inward))]
    from_whole = send(acc_whole, turned(direct))
    from_right = send(acc_right + from_far, turned(behind))
    from_left = [
        send(back[0] + acc_near[0], turned(outward)),
        send(back[1] + acc_near[1], turned(outward)),
    ]
    out = call(unpack_body, 6, [WHOLE], first=SMEM)(
        occupation, acc_home, from_right, from_whole, *from_left
    )[0]
    return out[None]


def solution(mesh):
    spec = P(("group", "blk"))
    return jax.shard_map(
        local,
        mesh=mesh,
        in_specs=(P(("group", "blk"), None, None), spec),
        out_specs=P(("group", "blk"), None, None),
        check_vma=False,
    )
```

```python
import jax
import jax.numpy as jnp
import numpy as np
from jax import lax
from jax.experimental import pallas as pl
from jax.experimental.pallas import tpu as pltpu
from jax.sharding import PartitionSpec as P

SIZE = 64
HALF = 32
ROWS = 36
BF = jnp.bfloat16
F32 = jnp.float32


def two_parts(matrix):
    high = np.asarray(matrix, np.float64).astype(BF)
    low = (np.asarray(matrix, np.float64) - high.astype(np.float64)).astype(BF)
    return high, low


def real_basis(points, freqs, period):
    place = np.arange(points)
    rows, marks = [], []
    for freq in freqs:
        waves = [np.cos(2 * np.pi * freq * place / period)]
        waves.append(np.sin(2 * np.pi * freq * place / period))
        for wave in waves:
            norm = np.sqrt(np.sum(wave * wave))
            if norm > 1e-6:
                rows.append(wave / norm)
                marks.append(freq)
    return np.stack(rows), np.asarray(marks, np.float64)


def left_form(matrix):
    high, low = two_parts(matrix)
    return np.concatenate([high, high, low], axis=1)


def right_form(matrix):
    high, low = two_parts(matrix)
    row = np.concatenate([high, low], axis=1)
    return np.concatenate([row, row], axis=0)


def constants():
    full, marks = real_basis(SIZE, range(HALF + 1), SIZE)
    even, even_marks = real_basis(HALF, range(0, HALF + 1, 2), SIZE)
    odd, odd_marks = real_basis(HALF, range(1, HALF, 2), SIZE)
    mix = np.array([[1.0, 1.0], [1.0, -1.0]]) / np.sqrt(2.0)
    lane = np.kron(mix, full)
    mid_marks = np.stack([even_marks, odd_marks], axis=1)
    total = (
        marks[:, None, None, None] ** 2
        + mid_marks[None, :, :, None] ** 2
        + marks[None, None, None, :] ** 2
    )
    step = 2.0 * np.pi / SIZE
    kernel = (np.pi / (step * step * total + 0.25)).astype(np.float32)
    kernel = kernel.reshape(SIZE * HALF, 2 * SIZE)
    parts = (
        left_form(full),
        left_form(full.T),
        right_form(lane.T),
        right_form(lane),
        left_form(np.concatenate([even, odd], axis=0)),
        left_form(np.concatenate([even.T, odd.T], axis=0)),
    )
    table = [np.pad(part, ((0, 0), (0, 256 - part.shape[1]))) for part in parts]
    return np.concatenate(table, axis=0), kernel


WHERE = {
    "fa": (0, 64, 192),
    "ba": (64, 64, 192),
    "fl": (128, 256, 256),
    "bl": (384, 256, 256),
    "fm": (640, 64, 96),
    "bm": (704, 64, 96),
}


def matrix(mats, name):
    start, rows, columns = WHERE[name]
    return mats[0][start : start + rows, :columns]


def split(value):
    high = value.astype(BF)
    low = (value - high.astype(F32)).astype(BF)
    return high, low


def along_rows(matrix, value):
    high, low = split(value)
    stack = jnp.concatenate([high, low, high], axis=0)
    return jnp.dot(matrix, stack, preferred_element_type=F32)


def along_lanes(value, matrix):
    high, low = split(value)
    both = jnp.dot(
        jnp.concatenate([high, low], axis=1), matrix, preferred_element_type=F32
    )
    return both[:, :128] + both[:, 128:]


def to_rows(value):
    count = value.shape[1] // 128
    return jnp.concatenate(
        [value[:, n * 128 : (n + 1) * 128] for n in range(count)], axis=0
    )


def to_lanes(value, rows):
    count = value.shape[0] // rows
    return jnp.concatenate(
        [value[n * rows : (n + 1) * rows] for n in range(count)], axis=1
    )


def pick(value):
    lane = lax.broadcasted_iota(jnp.int32, (HALF, value.shape[1]), 1)
    return jnp.where((lane & 127) < SIZE, value[:HALF], value[HALF:])


def take(refs, lanes):
    parts = [ref[:, lanes] for ref in refs]
    return parts[0] if len(parts) == 1 else jnp.concatenate(parts, axis=0)


def put(refs, lanes, value):
    refs[0][:, lanes] = value[:HALF]
    refs[1][:, lanes] = value[HALF:]


def skewed(first, second, edges, bases):
    prior = None
    for base in bases:
        for edge in edges:
            value = first(edge, base)
            if prior is not None:
                second(*prior)
            prior = (edge, base, value)
    second(*prior)


def solve(edges, mats, areas, tiles=16, count=32):
    waves, others = areas[: len(edges)], areas[len(edges) :]
    number = range(len(edges))
    kernel = mats[1]

    def rows_in(n, base):
        left, right, _ = edges[n]
        lanes = pl.ds(base * 128, tiles * 128)
        return along_rows(matrix(mats, "fa"), take(left, lanes) * take(right, lanes))

    def lanes_in(n, base, value):
        value = along_lanes(to_rows(value), matrix(mats, "fl"))
        for m in range(tiles):
            part = value[m * SIZE : (m + 1) * SIZE]
            waves[n][pl.ds(base + m, SIZE, stride=ROWS), :] = part

    def middle_in(n, base):
        rows = [waves[n][pl.ds((base + m) * ROWS, HALF), :] for m in range(count)]
        value = jnp.concatenate(rows, axis=1)
        value = pick(along_rows(matrix(mats, "fm"), value))
        return value * to_lanes(kernel[pl.ds(base * HALF, count * HALF), :], HALF)

    def middle_out(n, base, value):
        value = pick(along_rows(matrix(mats, "bm"), value))
        for m in range(count):
            part = value[:, m * 128 : (m + 1) * 128]
            others[n][pl.ds((base + m) * ROWS, HALF), :] = part

    def lanes_out(n, base):
        rows = [others[n][pl.ds(base + m, SIZE, stride=ROWS), :] for m in range(tiles)]
        return along_lanes(jnp.concatenate(rows, axis=0), matrix(mats, "bl"))

    def rows_out(n, base, value):
        left, right, finish = edges[n]
        value = along_rows(matrix(mats, "ba"), to_lanes(value, SIZE))
        lanes = pl.ds(base * 128, tiles * 128)
        finish(lanes, value * take(right, lanes), value * take(left, lanes))

    skewed(rows_in, lanes_in, number, range(0, HALF, tiles))
    skewed(middle_in, middle_out, number, range(0, SIZE, count))
    skewed(lanes_out, rows_out, number, range(0, HALF, tiles))


def pack_body(occ, orb, out, top, bottom):
    scale = jnp.sqrt(jnp.full((1, 128), occ[0], F32))
    low = lax.broadcasted_iota(jnp.int32, (SIZE, 128), 1) < SIZE
    for n in range(HALF // 2):
        first = orb[:, n * 128 : (n + 1) * 128] * scale
        second = orb[:, (n + 16) * 128 : (n + 17) * 128] * scale
        even = jnp.where(low, first, pltpu.roll(second, SIZE, 1))
        odd = jnp.where(low, pltpu.roll(first, SIZE, 1), second)
        for m, value in ((2 * n, even), (2 * n + 1, odd)):
            lanes = slice(m * 128, (m + 1) * 128)
            out[:, lanes] = value
            top[:, lanes] = value[:HALF]
            bottom[:, lanes] = value[HALF:]


def unpack_body(occ, one, two, top, bottom, out):
    scale = -lax.rsqrt(jnp.full((1, 128), occ[0], F32))
    low = lax.broadcasted_iota(jnp.int32, (SIZE, 128), 1) < SIZE
    for n in range(HALF // 2):
        parts = []
        for m in (2 * n, 2 * n + 1):
            lanes = slice(m * 128, (m + 1) * 128)
            three = take((top, bottom), lanes)
            parts.append((one[:, lanes] + two[:, lanes] + three) * scale)
        even, odd = parts
        out[:, n * 128 : (n + 1) * 128] = jnp.where(low, even, pltpu.roll(odd, SIZE, 1))
        out[:, (n + 16) * 128 : (n + 17) * 128] = jnp.where(
            low, pltpu.roll(even, SIZE, 1), odd
        )


WHOLE = jax.ShapeDtypeStruct((SIZE, SIZE * SIZE), F32)
PART = jax.ShapeDtypeStruct((HALF, SIZE * SIZE), F32)
SMEM = pl.BlockSpec(memory_space=pltpu.SMEM)
VMEM = pl.BlockSpec(memory_space=pltpu.VMEM)
COST = 2 * 6 * SIZE**4 * 200
AREA = pltpu.VMEM((SIZE * ROWS, 128), F32)


def call(body, count, outs, scratch=(), work=0, first=VMEM):
    return pl.pallas_call(
        body,
        out_shape=list(outs),
        in_specs=[first] + [VMEM] * (count - 1),
        out_specs=[VMEM] * len(outs),
        scratch_shapes=list(scratch),
        cost_estimate=pl.CostEstimate(
            flops=work * COST, bytes_accessed=1 << 20, transcendentals=0
        ),
        compiler_params=pltpu.CompilerParams(vmem_limit_bytes=28 << 20),
    )


def first_body(home, right, near_top, near_bottom, *rest):
    mats, outs = rest[:2], rest[2:]
    home_out, right_out, top_out, bottom_out, *areas = outs

    def finish_home(lanes, first, second):
        home_out[:, lanes] = first
        right_out[:, lanes] = second

    def finish_near(lanes, first, second):
        right_out[:, lanes] += second
        put((top_out, bottom_out), lanes, first)

    edges = (
        ((home,), (right,), finish_home),
        ((near_top, near_bottom), (right,), finish_near),
    )
    solve(edges, mats, areas)


def second_body(left_top, left_bottom, home, right, far, home_in, right_in, *rest):
    mats, outs = rest[:2], rest[2:]
    top_out, bottom_out, home_out, right_out, far_out, *areas = outs
    left, left_outs = (left_top, left_bottom), (top_out, bottom_out)

    def finish_far(lanes, first, second):
        put(left_outs, lanes, first)
        far_out[:, lanes] = second

    def finish_right(lanes, first, second):
        put(left_outs, lanes, take(left_outs, lanes) + first)
        right_out[:, lanes] = right_in[:, lanes] + second

    def finish_home(lanes, first, second):
        put(left_outs, lanes, take(left_outs, lanes) + first)
        home_out[:, lanes] = home_in[:, lanes] + second

    edges = (
        (left, (far,), finish_far),
        (left, (right,), finish_right),
        (left, (home,), finish_home),
    )
    solve(edges, mats, areas)


AXES = ("group", "blk")


def send(value, pairs):
    return lax.ppermute(value, AXES, pairs)


def routes(groups, blocks):
    def at(group, place):
        return (group % groups) * blocks + place % blocks

    outward, inward, across = [], [], []
    for group in range(groups):
        for place in range(blocks):
            source, target = at(group, place + 1), at(group, place)
            if group % 2:
                relay = at(group + 1, place + 1)
                across.append((at(group - 1, place), target))
            else:
                relay = at(group - 1, place)
            outward.append((source, relay))
            inward.append((relay, target))
    behind = [
        (at(group, place - 2), at(group, place))
        for group in range(groups)
        for place in range(blocks)
    ]
    return outward, inward, across, behind


def turned(pairs):
    return [(target, source) for source, target in pairs]


def local(orbitals, occupation):
    mats = [jnp.asarray(item) for item in constants()]
    groups, blocks = lax.axis_size("group"), lax.axis_size("blk")
    outward, inward, across, behind = routes(groups, blocks)
    odd = lax.axis_index("group") % 2 == 1
    home, top, bottom = call(pack_body, 2, [WHOLE, PART, PART], first=SMEM)(
        occupation, orbitals[0]
    )
    right = send(home, behind)
    near = [send(top, outward), send(bottom, outward)]
    left = [send(near[0], inward), send(near[1], inward)]
    far = send(right, across)
    near = [jnp.where(odd, part, 0.0) for part in near]
    acc_home, acc_right, *acc_near = call(
        first_body, 6, [WHOLE, WHOLE, PART, PART], [AREA] * 4, 2
    )(home, right, *near, *mats)
    *acc_left, acc_home, acc_right, acc_far = call(
        second_body, 9, [PART, PART, WHOLE, WHOLE, WHOLE], [AREA] * 6, 3
    )(*left, home, right, far, acc_home, acc_right, *mats)
    back = [send(acc_left[0], turned(inward)), send(acc_left[1], turned(inward))]
    from_far = send(acc_far, turned(across))
    from_right = send(acc_right + from_far, turned(behind))
    from_left = [
        send(back[0] + acc_near[0], turned(outward)),
        send(back[1] + acc_near[1], turned(outward)),
    ]
    out = call(unpack_body, 5, [WHOLE], first=SMEM)(
        occupation, acc_home, from_right, *from_left
    )[0]
    return out[None]


def solution(mesh):
    spec = P(("group", "blk"))
    return jax.shard_map(
        local,
        mesh=mesh,
        in_specs=(P(("group", "blk"), None, None), spec),
        out_specs=P(("group", "blk"), None, None),
        check_vma=False,
    )
```

```python
import jax
import jax.numpy as jnp
import numpy as np
from jax import lax
from jax.experimental import pallas as pl
from jax.experimental.pallas import tpu as pltpu
from jax.sharding import PartitionSpec as P

SIZE = 64
HALF = 32
ROWS = 36
BF = jnp.bfloat16
F32 = jnp.float32


def two_parts(matrix):
    high = np.asarray(matrix, np.float64).astype(BF)
    low = (np.asarray(matrix, np.float64) - high.astype(np.float64)).astype(BF)
    return high, low


def real_basis(points, freqs, period):
    place = np.arange(points)
    rows, marks = [], []
    for freq in freqs:
        waves = [np.cos(2 * np.pi * freq * place / period)]
        waves.append(np.sin(2 * np.pi * freq * place / period))
        for wave in waves:
            norm = np.sqrt(np.sum(wave * wave))
            if norm > 1e-6:
                rows.append(wave / norm)
                marks.append(freq)
    return np.stack(rows), np.asarray(marks, np.float64)


def left_form(matrix):
    high, low = two_parts(matrix)
    return np.concatenate([high, high, low], axis=1)


def right_form(matrix):
    high, low = two_parts(matrix)
    row = np.concatenate([high, low], axis=1)
    return np.concatenate([row, row], axis=0)


def constants():
    full, marks = real_basis(SIZE, range(HALF + 1), SIZE)
    even, even_marks = real_basis(HALF, range(0, HALF + 1, 2), SIZE)
    odd, odd_marks = real_basis(HALF, range(1, HALF, 2), SIZE)
    mix = np.array([[1.0, 1.0], [1.0, -1.0]]) / np.sqrt(2.0)
    lane = np.kron(mix, full)
    mid_marks = np.stack([even_marks, odd_marks], axis=1)
    total = (
        marks[:, None, None, None] ** 2
        + mid_marks[None, :, :, None] ** 2
        + marks[None, None, None, :] ** 2
    )
    step = 2.0 * np.pi / SIZE
    kernel = (np.pi / (step * step * total + 0.25)).astype(np.float32)
    kernel = kernel.reshape(SIZE * HALF, 2 * SIZE)
    parts = (
        left_form(full),
        left_form(full.T),
        right_form(lane.T),
        right_form(lane),
        left_form(np.concatenate([even, odd], axis=0)),
        left_form(np.concatenate([even.T, odd.T], axis=0)),
    )
    table = [np.pad(part, ((0, 0), (0, 256 - part.shape[1]))) for part in parts]
    return np.concatenate(table, axis=0), kernel


WHERE = {
    "fa": (0, 64, 192),
    "ba": (64, 64, 192),
    "fl": (128, 256, 256),
    "bl": (384, 256, 256),
    "fm": (640, 64, 96),
    "bm": (704, 64, 96),
}


def matrix(mats, name):
    start, rows, columns = WHERE[name]
    return mats[0][start : start + rows, :columns]


def split(value):
    high = value.astype(BF)
    low = (value - high.astype(F32)).astype(BF)
    return high, low


def along_rows(matrix, value):
    high, low = split(value)
    stack = jnp.concatenate([high, low, high], axis=0)
    return jnp.dot(matrix, stack, preferred_element_type=F32)


def along_lanes(value, matrix):
    high, low = split(value)
    both = jnp.dot(
        jnp.concatenate([high, low], axis=1), matrix, preferred_element_type=F32
    )
    return both[:, :128] + both[:, 128:]


def to_rows(value):
    count = value.shape[1] // 128
    return jnp.concatenate(
        [value[:, n * 128 : (n + 1) * 128] for n in range(count)], axis=0
    )


def to_lanes(value, rows):
    count = value.shape[0] // rows
    return jnp.concatenate(
        [value[n * rows : (n + 1) * rows] for n in range(count)], axis=1
    )


def pick(value):
    lane = lax.broadcasted_iota(jnp.int32, (HALF, value.shape[1]), 1)
    return jnp.where((lane & 127) < SIZE, value[:HALF], value[HALF:])


def take(refs, lanes):
    parts = [ref[:, lanes] for ref in refs]
    return parts[0] if len(parts) == 1 else jnp.concatenate(parts, axis=0)


def put(refs, lanes, value):
    refs[0][:, lanes] = value[:HALF]
    refs[1][:, lanes] = value[HALF:]


def skewed(first, second, edges, bases):
    prior = None
    for base in bases:
        for edge in edges:
            value = first(edge, base)
            if prior is not None:
                second(*prior)
            prior = (edge, base, value)
    second(*prior)


def solve(edges, mats, areas, tiles=16, count=32):
    waves, others = areas[: len(edges)], areas[len(edges) :]
    number = range(len(edges))
    kernel = mats[1]

    def rows_in(n, base):
        left, right, _ = edges[n]
        lanes = pl.ds(base * 128, tiles * 128)
        return along_rows(matrix(mats, "fa"), take(left, lanes) * take(right, lanes))

    def lanes_in(n, base, value):
        value = along_lanes(to_rows(value), matrix(mats, "fl"))
        for m in range(tiles):
            part = value[m * SIZE : (m + 1) * SIZE]
            waves[n][pl.ds(base + m, SIZE, stride=ROWS), :] = part

    def middle_in(n, base):
        rows = [waves[n][pl.ds((base + m) * ROWS, HALF), :] for m in range(count)]
        value = jnp.concatenate(rows, axis=1)
        value = pick(along_rows(matrix(mats, "fm"), value))
        return value * to_lanes(kernel[pl.ds(base * HALF, count * HALF), :], HALF)

    def middle_out(n, base, value):
        value = pick(along_rows(matrix(mats, "bm"), value))
        for m in range(count):
            part = value[:, m * 128 : (m + 1) * 128]
            others[n][pl.ds((base + m) * ROWS, HALF), :] = part

    def lanes_out(n, base):
        rows = [others[n][pl.ds(base + m, SIZE, stride=ROWS), :] for m in range(tiles)]
        return along_lanes(jnp.concatenate(rows, axis=0), matrix(mats, "bl"))

    def rows_out(n, base, value):
        left, right, finish = edges[n]
        value = along_rows(matrix(mats, "ba"), to_lanes(value, SIZE))
        lanes = pl.ds(base * 128, tiles * 128)
        finish(lanes, value * take(right, lanes), value * take(left, lanes))

    skewed(rows_in, lanes_in, number, range(0, HALF, tiles))
    skewed(middle_in, middle_out, number, range(0, SIZE, count))
    skewed(lanes_out, rows_out, number, range(0, HALF, tiles))


def pieces(left, right, sems):
    copies = []
    for n in range(8):
        lanes = pl.ds(n * 512, 512)
        copies.append(
            pltpu.make_async_copy(left.at[:, lanes], right.at[:, lanes], sems.at[n])
        )
    return copies


def pack_body(occ, orb, out, top, bottom):
    scale = jnp.sqrt(jnp.full((1, 128), occ[0], F32))
    low = lax.broadcasted_iota(jnp.int32, (SIZE, 128), 1) < SIZE
    for n in range(HALF // 2):
        first = orb[:, n * 128 : (n + 1) * 128] * scale
        second = orb[:, (n + 16) * 128 : (n + 17) * 128] * scale
        even = jnp.where(low, first, pltpu.roll(second, SIZE, 1))
        odd = jnp.where(low, pltpu.roll(first, SIZE, 1), second)
        for m, value in ((2 * n, even), (2 * n + 1, odd)):
            lanes = slice(m * 128, (m + 1) * 128)
            out[:, lanes] = value
            top[:, lanes] = value[:HALF]
            bottom[:, lanes] = value[HALF:]


def unpack_body(occ, one, two, top, bottom, target, out, sems):
    copies = pieces(out, target, sems)
    scale = -lax.rsqrt(jnp.full((1, 128), occ[0], F32))
    low = lax.broadcasted_iota(jnp.int32, (SIZE, 128), 1) < SIZE
    for n in range(HALF // 2):
        parts = []
        for m in (2 * n, 2 * n + 1):
            lanes = slice(m * 128, (m + 1) * 128)
            three = take((top, bottom), lanes)
            parts.append((one[:, lanes] + two[:, lanes] + three) * scale)
        even, odd = parts
        out[:, n * 128 : (n + 1) * 128] = jnp.where(low, even, pltpu.roll(odd, SIZE, 1))
        out[:, (n + 16) * 128 : (n + 17) * 128] = jnp.where(
            low, pltpu.roll(even, SIZE, 1), odd
        )
        if n % 4 == 3:
            copies[n // 4].start()
            copies[n // 4 + 4].start()
    for copy in copies:
        copy.wait()


WHOLE = jax.ShapeDtypeStruct((SIZE, SIZE * SIZE), F32)
PART = jax.ShapeDtypeStruct((HALF, SIZE * SIZE), F32)
SMEM = pl.BlockSpec(memory_space=pltpu.SMEM)
VMEM = pl.BlockSpec(memory_space=pltpu.VMEM)
COST = 2 * 6 * SIZE**4 * 200
HBM = pl.BlockSpec(memory_space=pltpu.HBM)
MOVE = (pltpu.VMEM((SIZE, SIZE * SIZE), F32), pltpu.SemaphoreType.DMA((8,)))
AREA = pltpu.VMEM((SIZE * ROWS, 128), F32)


def call(body, count, outs, scratch=(), work=0, first=VMEM, out=VMEM):
    return pl.pallas_call(
        body,
        out_shape=list(outs),
        in_specs=[first] + [VMEM] * (count - 1),
        out_specs=[out] * len(outs),
        scratch_shapes=list(scratch),
        cost_estimate=pl.CostEstimate(
            flops=work * COST, bytes_accessed=1 << 20, transcendentals=0
        ),
        compiler_params=pltpu.CompilerParams(vmem_limit_bytes=28 << 20),
    )


def first_body(home, right, near_top, near_bottom, *rest):
    mats, outs = rest[:2], rest[2:]
    home_out, right_out, top_out, bottom_out, *areas = outs

    def finish_home(lanes, first, second):
        home_out[:, lanes] = first
        right_out[:, lanes] = second

    def finish_near(lanes, first, second):
        right_out[:, lanes] += second
        put((top_out, bottom_out), lanes, first)

    edges = (
        ((home,), (right,), finish_home),
        ((near_top, near_bottom), (right,), finish_near),
    )
    solve(edges, mats, areas)


def second_body(left_top, left_bottom, home, right, far, home_in, right_in, *rest):
    mats, outs = rest[:2], rest[2:]
    top_out, bottom_out, home_out, right_out, far_out, *areas = outs
    left, left_outs = (left_top, left_bottom), (top_out, bottom_out)

    def finish_far(lanes, first, second):
        put(left_outs, lanes, first)
        far_out[:, lanes] = second

    def finish_right(lanes, first, second):
        put(left_outs, lanes, take(left_outs, lanes) + first)
        right_out[:, lanes] = right_in[:, lanes] + second

    def finish_home(lanes, first, second):
        put(left_outs, lanes, take(left_outs, lanes) + first)
        home_out[:, lanes] = home_in[:, lanes] + second

    edges = (
        (left, (far,), finish_far),
        (left, (right,), finish_right),
        (left, (home,), finish_home),
    )
    solve(edges, mats, areas)


AXES = ("group", "blk")


def send(value, pairs):
    return lax.ppermute(value, AXES, pairs)


def routes(groups, blocks):
    def at(group, place):
        return (group % groups) * blocks + place % blocks

    outward, inward, across = [], [], []
    for group in range(groups):
        for place in range(blocks):
            source, target = at(group, place + 1), at(group, place)
            if group % 2:
                relay = at(group + 1, place + 1)
                across.append((at(group - 1, place), target))
            else:
                relay = at(group - 1, place)
            outward.append((source, relay))
            inward.append((relay, target))
    behind = [
        (at(group, place - 2), at(group, place))
        for group in range(groups)
        for place in range(blocks)
    ]
    return outward, inward, across, behind


def turned(pairs):
    return [(target, source) for source, target in pairs]


def local(orbitals, occupation):
    mats = [jnp.asarray(item) for item in constants()]
    groups, blocks = lax.axis_size("group"), lax.axis_size("blk")
    outward, inward, across, behind = routes(groups, blocks)
    odd = lax.axis_index("group") % 2 == 1
    home, top, bottom = call(pack_body, 2, [WHOLE, PART, PART], first=SMEM)(
        occupation, orbitals[0]
    )
    right = send(home, behind)
    near = [send(top, outward), send(bottom, outward)]
    left = [send(near[0], inward), send(near[1], inward)]
    far = send(right, across)
    near = [jnp.where(odd, part, 0.0) for part in near]
    acc_home, acc_right, *acc_near = call(
        first_body, 6, [WHOLE, WHOLE, PART, PART], [AREA] * 4, 2
    )(home, right, *near, *mats)
    *acc_left, acc_home, acc_right, acc_far = call(
        second_body, 9, [PART, PART, WHOLE, WHOLE, WHOLE], [AREA] * 6, 3
    )(*left, home, right, far, acc_home, acc_right, *mats)
    back = [send(acc_left[0], turned(inward)), send(acc_left[1], turned(inward))]
    from_far = send(acc_far, turned(across))
    from_right = send(acc_right + from_far, turned(behind))
    from_left = [
        send(back[0] + acc_near[0], turned(outward)),
        send(back[1] + acc_near[1], turned(outward)),
    ]
    out = call(unpack_body, 5, [WHOLE], MOVE, first=SMEM, out=HBM)(
        occupation, acc_home, from_right, *from_left
    )[0]
    return out[None]


def solution(mesh):
    spec = P(("group", "blk"))
    return jax.shard_map(
        local,
        mesh=mesh,
        in_specs=(P(("group", "blk"), None, None), spec),
        out_specs=P(("group", "blk"), None, None),
        check_vma=False,
    )
```
